32 devices in a mesh: gx: 8 (over z, x), gy: 4 (over y, core).
Axes of the slice: x: 2, y: 2, z: 4, core: 2. Of those that a mesh axis runs over, the one named last changes fastest.
Arguments:
- orbitals: bfloat16 [20000, 200], P('gx'), may hold values from -6 to 6
- projector: bfloat16 [6016, 20000], P('gy', 'gx'), may hold values from -0.0390625 to 0.0390625
- integrals: bfloat16 [8, 6016, 6016], P('gx', 'gy'), may hold values from -1 to 1
Outputs:
- exchange_matrix: float32 [6016, 6016], P('gx', 'gy')
- exchange_orbitals: float32 [20000, 200], P('gx', 'gy')
- energy_mean: float32 [], replicated
- trace_mean: float32 [], replicated
The draws below stay inside these ranges and needn't reach their ends.
All inputs are finite; a program needn't handle non-finite values.
Results may differ from the reference program's by a relative error of at most 0.008.
Values may be sent and summed in bfloat16 or wider, within the bound.
No kernel may reach another device: no remote copies, remote signals or barrier semaphores. Data moves between devices by JAX's collectives and lax.ppermute only.
A program may use at most 128 MiB of HBM per device.

```python
import jax
import jax.numpy as jnp
from jax import lax

NAO = 20000
NADM = 6016
NOCC = 200
NAUX = 8


def draw_integrals(key, part):
    keyed = jax.random.fold_in(key, 11)
    first = jax.random.fold_in(keyed, 0)
    shape = (NAUX, NADM, NADM)
    base = jax.random.normal(first, shape, jnp.float32)
    aux_scale = 0.5 + jnp.arange(NAUX, dtype=jnp.float32) / max(NAUX - 1, 1)
    row_scale = 0.5 + jnp.arange(NADM, dtype=jnp.float32) / max(NADM - 1, 1)
    sigma = (NADM * NOCC * NAUX) ** (-0.5)
    values = base * aux_scale[:, None, None] * row_scale[None, :, None] * sigma
    return jnp.clip(values, -1.0, 1.0).astype(jnp.bfloat16)


def block_scale(rng, shape, cuts, smallest, high):
    factor_of, own = 1.0, jax.random.fold_in(rng, 6)
    for axis_at, blocks in cuts:
        heights = jnp.exp(jax.random.uniform(jax.random.fold_in(own, axis_at), (blocks,), jnp.float32, smallest / len(cuts), high / len(cuts)))
        factor_of = factor_of * jnp.repeat(heights, shape[axis_at] // blocks).reshape([-1 if axis == axis_at else 1 for axis in range(len(shape))])
    return factor_of


def gaussian(rng, dims, width, reach, pieces=(), kind=jnp.bfloat16):
    gain = block_scale(rng, dims, pieces, -0.22, 0.18) if pieces else 1.0
    drawn = jax.random.normal(rng, dims, jnp.float32) * width * gain
    return jnp.minimum(jnp.maximum(drawn, -reach), reach).astype(kind)


def setup_inputs(seed: int = 0) -> dict:
    splits = jax.random.split(jax.random.key(seed), 4)
    return {
        "orbitals": gaussian(splits[0], (NAO, NOCC), 1.0, 6.0, ((0, 8),)),
        "projector": gaussian(splits[1], (NADM, NAO), NAO ** -0.5, 0.0390625, ((0, 4), (1, 8))),
        "integrals": draw_integrals(jax.random.fold_in(splits[3], 71), 0),
    }


def reference(orbitals, projector, integrals):
    admm = jnp.dot(projector, orbitals, preferred_element_type=jnp.float32).astype(jnp.bfloat16)

    def transform(slab):
        return jnp.dot(slab, admm, preferred_element_type=jnp.float32).astype(jnp.bfloat16)

    half = lax.map(transform, integrals)
    merged = jnp.transpose(half, (1, 0, 2)).reshape(NADM, NAUX * NOCC)
    exchange = jnp.dot(merged, merged.T, preferred_element_type=jnp.float32)
    admm_wide = admm.astype(jnp.float32)
    applied = jnp.dot(exchange, admm_wide, precision=lax.Precision.HIGHEST)
    applied_low = applied.astype(jnp.bfloat16)
    back = jnp.dot(projector.T, applied_low, preferred_element_type=jnp.float32)
    energy = -0.5 * jnp.sum(admm_wide * applied) / (NADM * NOCC)
    trace = jnp.sum(jnp.diagonal(exchange)) / NADM
    return exchange, back, energy, trace
```

```python
import jax
import jax.numpy as jnp
from jax import lax
from jax.sharding import PartitionSpec as P


F32 = jnp.float32
BF16 = jnp.bfloat16

X_SWAP = [(i, i ^ 1) for i in range(8)]
CORE_SWAP = [(i, i ^ 1) for i in range(4)]
Y_SWAP = [(i, i ^ 2) for i in range(4)]


def along_z(pairs):
    return [(2 * a + x, 2 * b + x) for a, b in pairs for x in range(2)]


def z_mix(k):
    return along_z([(z, z ^ k) for z in range(4)])


def dot(a, b, dims):
    return lax.dot_general(a, b, (dims, ((), ())), preferred_element_type=F32)


def ordered(first, own, received):
    return jnp.where(
        first, jnp.stack([own, received]), jnp.stack([received, own])
    )


def pick(array, index):
    return lax.dynamic_index_in_dim(array, index, 0, keepdims=False)


def line_gather(own, z):
    up1 = lax.ppermute(own, "gx", along_z([(0, 1), (1, 2), (2, 3)]))
    down1 = lax.ppermute(own, "gx", along_z([(1, 0), (2, 1), (3, 2)]))
    up2 = lax.ppermute(up1, "gx", along_z([(1, 2), (2, 3)]))
    down2 = lax.ppermute(down1, "gx", along_z([(2, 1), (1, 0)]))
    up3 = lax.ppermute(up2, "gx", along_z([(2, 3)]))
    down3 = lax.ppermute(down2, "gx", along_z([(1, 0)]))
    near = jnp.where(z % 2 == 0, down1, up1)
    middle = jnp.where(
        z == 0, down2, jnp.where(z == 1, down1, jnp.where(z == 2, up1, up2))
    )
    far = jnp.where(
        z == 0, down3, jnp.where(z == 1, down2, jnp.where(z == 2, up2, up3))
    )
    blocks = []
    for block in (own, near, middle, far):
        blocks += [block, lax.ppermute(block, "gx", X_SWAP)]
    return blocks


def on_device(orbitals, projector, integrals):
    index_x = lax.axis_index("gx")
    index_y = lax.axis_index("gy")
    z, x = index_x // 2, index_x % 2
    y, core = index_y // 2, index_y % 2
    part_rows, total_adm = projector.shape[0], integrals.shape[2]
    nocc = orbitals.shape[1]
    block_rows = total_adm // 8
    piece = -(-part_rows // 8 // 32) * 32
    partial_value = dot(projector, orbitals, ((1,), (0,)))
    partial_value = jnp.pad(partial_value, ((0, 8 * piece - part_rows), (0, 0)))
    partial_value = partial_value.reshape(2, 4, piece, nocc)
    got = lax.ppermute(pick(partial_value, 1 - x).astype(BF16), "gx", X_SWAP)
    partial_value = pick(partial_value, x) + got.astype(F32)
    partial_low = partial_value.astype(BF16)
    total = pick(partial_value, z)
    for k in range(1, 4):
        got = lax.ppermute(pick(partial_low, z ^ k), "gx", z_mix(k))
        total = total + got.astype(F32)
    own = total.astype(BF16)
    line = jnp.zeros((4, piece, nocc), BF16)
    line = lax.dynamic_update_index_in_dim(line, own, z, 0)
    for k in range(1, 4):
        got = lax.ppermute(own, "gx", z_mix(k))
        line = lax.dynamic_update_index_in_dim(line, got, z ^ k, 0)
    cut = piece // 2
    one, two = line[:, :cut], line[:, cut:]
    one = ordered(x == 0, one, lax.ppermute(one, "gx", X_SWAP))
    two = ordered(y == 0, two, lax.ppermute(two, "gy", Y_SWAP))
    one = ordered(y == 0, one, lax.ppermute(one, "gy", Y_SWAP))
    two = jnp.swapaxes(ordered(x == 0, two, lax.ppermute(two, "gx", X_SWAP)), 0, 1)
    both = jnp.concatenate([one, two], axis=3)
    both = both.reshape(2, 8 * piece, nocc)
    admm = ordered(core == 0, both, lax.ppermute(both, "gy", CORE_SWAP))
    admm = jnp.swapaxes(admm, 0, 1)[:, :, :part_rows].reshape(total_adm, nocc)

    half = dot(admm, integrals[0], ((0,), (1,))).astype(BF16)
    half_wide = half.astype(F32)
    trace_part = jnp.sum(half_wide * half_wide)
    rows_admm = lax.dynamic_slice_in_dim(admm, index_y * part_rows, part_rows, 0)
    inner = dot(half, rows_admm, ((1,), (0,)))
    inner_rows = -(-(nocc + 1) // 16) * 8
    tail = jnp.zeros((2 * inner_rows - nocc, nocc), F32).at[0].set(trace_part)
    inner = jnp.concatenate([inner, tail]).reshape(2, inner_rows, nocc)
    inner = pick(inner, core) + lax.ppermute(pick(inner, 1 - core), "gy", CORE_SWAP)
    inner = inner + lax.ppermute(inner, "gy", Y_SWAP)
    rounded = lax.reduce_precision(inner, 8, 7)
    rest = inner - rounded
    last = nocc - inner_rows
    inner = rounded.at[last + 1].set(
        jnp.where(core == 1, rest[last], rounded[last + 1])
    )
    inner = inner.astype(BF16)

    halves = line_gather(half, z)
    inners = jnp.stack(line_gather(inner, z))
    inners = ordered(core == 0, inners, lax.ppermute(inners, "gy", CORE_SWAP))

    root_y, root_core = z // 2, z % 2
    low_rows = nocc // 2 // 16 * 16
    row_blocks = []
    high_rows = nocc - low_rows
    for pair in range(4):
        block = jnp.stack(halves[2 * pair : 2 * pair + 2])
        block = jnp.where(
            x == 0, block[:, :, :block_rows], block[:, :, part_rows - block_rows :]
        )
        passed = lax.ppermute(block, "gy", CORE_SWAP)
        block = jnp.where(core == root_core, block, passed)
        mine = jnp.where(core == 0, block[:, :high_rows], block[:, low_rows:])
        passed = lax.ppermute(mine, "gy", Y_SWAP)
        mine = jnp.where(y == root_y, mine, passed)
        other = lax.ppermute(mine, "gy", CORE_SWAP)
        low = jnp.where(core == 0, mine, other)
        high = jnp.where(core == 0, other, mine)
        row_blocks += [low, high[:, high_rows - low_rows :]]
        row_blocks[-2:] = [jnp.concatenate(row_blocks[-2:], axis=1)]
    rows = jnp.concatenate(row_blocks).reshape(8 * nocc, block_rows)
    columns = jnp.concatenate(halves)
    exchange = dot(rows, columns, ((0,), (0,)))

    weights = jnp.swapaxes(inners, 0, 1).reshape(8, 2 * inner_rows, nocc)
    applied = dot(columns, weights[:, :nocc].reshape(8 * nocc, nocc), ((0,), (0,)))
    applied_low = applied.astype(BF16)
    back = dot(applied_low, projector, ((0,), (0,)))
    back = back.reshape(2, 2, nocc // 4, projector.shape[1])
    keep = lax.dynamic_index_in_dim(back, core, 1, keepdims=False)
    give = lax.dynamic_index_in_dim(back, 1 - core, 1, keepdims=False).astype(BF16)
    back = keep + lax.ppermute(give, "gy", CORE_SWAP).astype(F32)
    got = lax.ppermute(pick(back, 1 - y).astype(BF16), "gy", Y_SWAP)
    back = (pick(back, y) + got.astype(F32)).T

    wide = weights.astype(F32)
    energies = jnp.sum(wide[:, :nocc] * wide[:, :nocc], axis=(1, 2))
    traces = wide[:, nocc, 0] + wide[:, nocc + 1, 0]
    slot = jnp.arange(8)
    near_z = jnp.array([[0, 1, 2, 3], [1, 0, 2, 3], [2, 3, 1, 0], [3, 2, 1, 0]])
    holder = pick(near_z, z)[slot // 2] * 2 + (x ^ (slot % 2))
    place = holder[:, None] == slot[None, :]
    energies = jnp.sum(jnp.where(place, energies[:, None], 0.0), axis=0)
    traces = jnp.sum(jnp.where(place, traces[:, None], 0.0), axis=0)
    energy_mean = -0.5 * jnp.sum(energies) / (total_adm * nocc)
    trace_mean = jnp.sum(traces) / total_adm
    return (exchange, back, energy_mean, trace_mean)


def any_mesh(orbitals, projector, integrals):
    part_rows = projector.shape[0]
    partial_value = dot(projector, orbitals, ((1,), (0,)))
    own_admm = lax.psum(partial_value, "gx").astype(BF16)
    admm = lax.all_gather(own_admm, "gy", axis=0, tiled=True)
    total_adm, nocc = admm.shape
    half = dot(integrals, admm, ((2,), (0,))).astype(BF16)
    block_rows = total_adm // lax.axis_size("gx")
    first_row = lax.axis_index("gx") * block_rows
    index_y = lax.axis_index("gy")
    all_half = lax.all_gather(half, "gx", axis=0, tiled=True)
    offset = jnp.clip(first_row - index_y * part_rows, 0, part_rows - block_rows)
    mine = lax.dynamic_slice_in_dim(all_half, offset, block_rows, 1)
    mine = jnp.where(index_y == first_row // part_rows, mine, jnp.zeros_like(mine))
    rows = lax.psum(mine, "gy")
    exchange = dot(rows, all_half, ((0, 2), (0, 2)))
    own_rows = lax.dynamic_slice_in_dim(admm, index_y * part_rows, part_rows, 0)
    inner = lax.psum(dot(all_half, own_rows, ((1,), (0,))), "gy")
    wide = all_half.astype(F32)
    trace_mean = lax.psum(jnp.sum(wide * wide), "gy") / total_adm
    energy_mean = -0.5 * jnp.sum(inner * inner) / (total_adm * nocc)
    applied = dot(all_half, inner.astype(BF16), ((0, 2), (0, 1)))
    back_part = dot(projector, applied.astype(BF16), ((0,), (0,)))
    back = lax.psum_scatter(back_part, "gy", scatter_dimension=1, tiled=True)
    return (exchange, back, energy_mean, trace_mean)


def solution(mesh):
    fits = mesh.shape["gx"] == 8 and mesh.shape["gy"] == 4
    return jax.shard_map(
        on_device if fits else any_mesh,
        mesh=mesh,
        in_specs=(P("gx", None), P("gy", "gx"), P("gx", "gy", None)),
        out_specs=(P("gx", "gy"), P("gx", "gy"), P(), P()),
        check_vma=False,
    )
```

```python
import jax
import jax.numpy as jnp
from jax import lax
from jax.experimental.layout import Layout, with_layout_constraint
from jax.sharding import PartitionSpec as P


F32 = jnp.float32
BF16 = jnp.bfloat16

X_SWAP = [(i, i ^ 1) for i in range(8)]
CORE_SWAP = [(i, i ^ 1) for i in range(4)]
Y_SWAP = [(i, i ^ 2) for i in range(4)]


def along_z(pairs):
    return [(2 * a + x, 2 * b + x) for a, b in pairs for x in range(2)]


def z_mix(k):
    return along_z([(z, z ^ k) for z in range(4)])


def dot(a, b, dims):
    return lax.dot_general(a, b, (dims, ((), ())), preferred_element_type=F32)


def ordered(first, own, received):
    return jnp.where(
        first, jnp.stack([own, received]), jnp.stack([received, own])
    )


def pick(array, index):
    return lax.dynamic_index_in_dim(array, index, 0, keepdims=False)


def row_major(array):
    return with_layout_constraint(array, Layout(tuple(range(array.ndim))))


def first_steps(own):
    up1 = lax.ppermute(own, "gx", along_z([(0, 1), (1, 2), (2, 3)]))
    down1 = lax.ppermute(own, "gx", along_z([(1, 0), (2, 1), (3, 2)]))
    return up1, down1, lax.ppermute(own, "gx", X_SWAP)


def line_gather(own, z, steps=None):
    up1, down1, beside = steps or first_steps(own)
    up2 = lax.ppermute(up1, "gx", along_z([(1, 2), (2, 3)]))
    down2 = lax.ppermute(down1, "gx", along_z([(2, 1), (1, 0)]))
    up3 = lax.ppermute(up2, "gx", along_z([(2, 3)]))
    down3 = lax.ppermute(down2, "gx", along_z([(1, 0)]))
    near = jnp.where(z % 2 == 0, down1, up1)
    middle = jnp.where(
        z == 0, down2, jnp.where(z == 1, down1, jnp.where(z == 2, up1, up2))
    )
    far = jnp.where(
        z == 0, down3, jnp.where(z == 1, down2, jnp.where(z == 2, up2, up3))
    )
    blocks = [own, beside]
    for block in (near, middle, far):
        blocks += [block, lax.ppermute(block, "gx", X_SWAP)]
    return blocks


def on_device(orbitals, projector, integrals):
    index_x = lax.axis_index("gx")
    index_y = lax.axis_index("gy")
    z, x = index_x // 2, index_x % 2
    y, core = index_y // 2, index_y % 2
    part_rows, total_adm = projector.shape[0], integrals.shape[2]
    nocc = orbitals.shape[1]
    block_rows = total_adm // 8
    piece = -(-part_rows // 8 // 32) * 32
    partial_value = dot(projector, orbitals, ((1,), (0,)))
    partial_value = jnp.pad(partial_value, ((0, 8 * piece - part_rows), (0, 0)))
    partial_value = row_major(partial_value.reshape(2, 4, piece, nocc))
    got = lax.ppermute(pick(partial_value, 1 - x).astype(BF16), "gx", X_SWAP)
    partial_value = pick(partial_value, x) + got.astype(F32)
    partial_low = partial_value.astype(BF16)
    total = pick(partial_value, z)
    for k in range(1, 4):
        got = lax.ppermute(pick(partial_low, z ^ k), "gx", z_mix(k))
        total = total + got.astype(F32)
    own = total.astype(BF16)
    own = row_major(own)
    got = [lax.ppermute(own, "gx", z_mix(k)) for k in range(1, 4)]
    by_distance = [own] + got
    line = []
    for place in range(4):
        far_half = jnp.where(
            z == place ^ 3, by_distance[3], jnp.where(z == place ^ 2, by_distance[2], by_distance[1])
        )
        line.append(jnp.where(z == place, own, far_half))
    line = row_major(jnp.stack(line))
    cut = piece // 2
    one, two = line[:, :cut], line[:, cut:]
    one = ordered(x == 0, one, lax.ppermute(one, "gx", X_SWAP))
    two = ordered(y == 0, two, lax.ppermute(two, "gy", Y_SWAP))
    one = ordered(y == 0, one, lax.ppermute(one, "gy", Y_SWAP))
    two = jnp.swapaxes(ordered(x == 0, two, lax.ppermute(two, "gx", X_SWAP)), 0, 1)
    both = jnp.concatenate([one, two], axis=3)
    both = row_major(both.reshape(2, 8 * piece, nocc))
    got = row_major(lax.ppermute(both, "gy", CORE_SWAP))
    admm = row_major(ordered(core == 0, both, got))
    admm = jnp.swapaxes(admm, 0, 1)[:, :, :part_rows]
    admm = row_major(admm.reshape(total_adm, nocc))

    half = dot(admm, integrals[0], ((0,), (1,))).astype(BF16)
    steps = first_steps(half)
    half_late, steps = lax.optimization_barrier((half, steps))
    half_wide = half_late.astype(F32)
    trace_part = jnp.sum(half_wide * half_wide)
    rows_admm = lax.dynamic_slice_in_dim(admm, index_y * part_rows, part_rows, 0)
    inner = dot(half_late, rows_admm, ((1,), (0,)))
    inner_rows = -(-(nocc + 1) // 16) * 8
    tail = jnp.zeros((2 * inner_rows - nocc, nocc), F32).at[0].set(trace_part)
    inner = jnp.concatenate([inner, tail]).reshape(2, inner_rows, nocc)
    inner = pick(inner, core) + lax.ppermute(pick(inner, 1 - core), "gy", CORE_SWAP)
    inner = inner + lax.ppermute(inner, "gy", Y_SWAP)
    rounded = lax.reduce_precision(inner, 8, 7)
    rest = inner - rounded
    last = nocc - inner_rows
    inner = rounded.at[last + 1].set(
        jnp.where(core == 1, rest[last], rounded[last + 1])
    )
    inner = inner.astype(BF16)

    halves = line_gather(half, z, steps)
    inners = jnp.stack(line_gather(inner, z))
    inners = ordered(core == 0, inners, lax.ppermute(inners, "gy", CORE_SWAP))

    root_y, root_core = z // 2, z % 2
    low_rows = nocc // 2 // 16 * 16
    row_blocks = []
    high_rows = nocc - low_rows
    for pair in range(4):
        block = jnp.stack(halves[2 * pair : 2 * pair + 2])
        block = jnp.where(
            x == 0, block[:, :, :block_rows], block[:, :, part_rows - block_rows :]
        )
        passed = lax.ppermute(block, "gy", CORE_SWAP)
        block = jnp.where(core == root_core, block, passed)
        mine = jnp.where(core == 0, block[:, :high_rows], block[:, low_rows:])
        sent = mine
        passed = lax.ppermute(mine, "gy", Y_SWAP)
        mine = jnp.where(y == root_y, mine, passed)
        other = lax.ppermute(mine, "gy", CORE_SWAP)
        low = jnp.where(core == 0, mine, other)
        high = jnp.where(core == 0, other, mine)
        row_blocks += [low, high[:, high_rows - low_rows :]]
        row_blocks[-2:] = [jnp.concatenate(row_blocks[-2:], axis=1)]
    rows = jnp.concatenate(row_blocks).reshape(8 * nocc, block_rows)
    columns = jnp.concatenate(halves)
    exchange = dot(rows, columns, ((0,), (0,)))

    inners, _ = lax.optimization_barrier((inners, sent))
    weights = jnp.swapaxes(inners, 0, 1).reshape(8, 2 * inner_rows, nocc)
    applied = dot(columns, weights[:, :nocc].reshape(8 * nocc, nocc), ((0,), (0,)))
    applied_low = applied.astype(BF16)
    back = dot(applied_low, projector, ((0,), (0,)))
    back = back.reshape(2, 2, nocc // 4, projector.shape[1])
    keep = lax.dynamic_index_in_dim(back, core, 1, keepdims=False)
    give = lax.dynamic_index_in_dim(back, 1 - core, 1, keepdims=False).astype(BF16)
    back = keep + lax.ppermute(give, "gy", CORE_SWAP).astype(F32)
    got = lax.ppermute(pick(back, 1 - y).astype(BF16), "gy", Y_SWAP)
    back = (pick(back, y) + got.astype(F32)).T

    wide = weights.astype(F32)
    energies = jnp.sum(wide[:, :nocc] * wide[:, :nocc], axis=(1, 2))
    traces = wide[:, nocc, 0] + wide[:, nocc + 1, 0]
    slot = jnp.arange(8)
    near_z = jnp.array([[0, 1, 2, 3], [1, 0, 2, 3], [2, 3, 1, 0], [3, 2, 1, 0]])
    holder = pick(near_z, z)[slot // 2] * 2 + (x ^ (slot % 2))
    place = holder[:, None] == slot[None, :]
    energies = jnp.sum(jnp.where(place, energies[:, None], 0.0), axis=0)
    traces = jnp.sum(jnp.where(place, traces[:, None], 0.0), axis=0)
    energy_mean = -0.5 * jnp.sum(energies) / (total_adm * nocc)
    trace_mean = jnp.sum(traces) / total_adm
    return (exchange, back, energy_mean, trace_mean)


def any_mesh(orbitals, projector, integrals):
    part_rows = projector.shape[0]
    partial_value = dot(projector, orbitals, ((1,), (0,)))
    own_admm = lax.psum(partial_value, "gx").astype(BF16)
    admm = lax.all_gather(own_admm, "gy", axis=0, tiled=True)
    total_adm, nocc = admm.shape
    half = dot(integrals, admm, ((2,), (0,))).astype(BF16)
    block_rows = total_adm // lax.axis_size("gx")
    first_row = lax.axis_index("gx") * block_rows
    index_y = lax.axis_index("gy")
    all_half = lax.all_gather(half, "gx", axis=0, tiled=True)
    offset = jnp.clip(first_row - index_y * part_rows, 0, part_rows - block_rows)
    mine = lax.dynamic_slice_in_dim(all_half, offset, block_rows, 1)
    mine = jnp.where(index_y == first_row // part_rows, mine, jnp.zeros_like(mine))
    rows = lax.psum(mine, "gy")
    exchange = dot(rows, all_half, ((0, 2), (0, 2)))
    own_rows = lax.dynamic_slice_in_dim(admm, index_y * part_rows, part_rows, 0)
    inner = lax.psum(dot(all_half, own_rows, ((1,), (0,))), "gy")
    wide = all_half.astype(F32)
    trace_mean = lax.psum(jnp.sum(wide * wide), "gy") / total_adm
    energy_mean = -0.5 * jnp.sum(inner * inner) / (total_adm * nocc)
    applied = dot(all_half, inner.astype(BF16), ((0, 2), (0, 1)))
    back_part = dot(projector, applied.astype(BF16), ((0,), (0,)))
    back = lax.psum_scatter(back_part, "gy", scatter_dimension=1, tiled=True)
    return (exchange, back, energy_mean, trace_mean)


def solution(mesh):
    fits = mesh.shape["gx"] == 8 and mesh.shape["gy"] == 4
    return jax.shard_map(
        on_device if fits else any_mesh,
        mesh=mesh,
        in_specs=(P("gx", None), P("gy", "gx"), P("gx", "gy", None)),
        out_specs=(P("gx", "gy"), P("gx", "gy"), P(), P()),
        check_vma=False,
    )
```
